32 devices in a mesh: batch: 16 (over z, y, core), gene: 2 (over x).
Axes of the slice: x: 2, y: 2, z: 4, core: 2. Of those that a mesh axis runs over, the one named last changes fastest.
Arguments:
- umi_counts: int32 [16384, 8192], P('batch', 'gene'), may hold values from 0 to 65535
- cell_donors: int32 [16384], P('batch'), may hold values from 0 to 127
- cell_types: int32 [16384], P('batch'), may hold values from 0 to 23
- live_cells: int32 [16], P('batch'), may hold values from 1 to 1024, 10240 in all
- dosages: int32 [128, 2048], P(None, 'batch'), may hold values from 0 to 2
Outputs:
- scores: bfloat16 [24, 8192, 2048], P(None, ('gene', 'batch'))
The draws below stay inside these ranges and needn't reach their ends.
All inputs are finite; a program needn't handle non-finite values. No bound on the sum of `live_cells` on one device may be relied on, other than what follows from the above.
Results may differ from the reference program's by a relative error of at most 0.0069.
Values may be sent and summed in bfloat16 or wider, within the bound.
A program may use at most 128 MiB of HBM per device.

```python
import math
import jax
import jax.numpy as jnp
import numpy as np
from jax import lax

GENES = 8192
TYPES = 24
DONORS = 128
CELL_DEV = 1024
CELLS = 16384
VARIANTS = 2048
N_BATCH = 16


def draw_umi_counts(key, part):
    counts_key = jax.random.fold_in(key, 11)
    depth_key = jax.random.fold_in(key, 23)
    raw_counts = jax.random.randint(counts_key, (CELLS, GENES), 0, 65536, dtype=jnp.int32)
    depth_shift = jax.random.randint(depth_key, (CELLS, 1), 0, 4, dtype=jnp.int32)
    divisor = jnp.left_shift(jnp.ones_like(depth_shift), depth_shift)
    return jnp.floor_divide(raw_counts, divisor).astype(jnp.int32)


def set_ends(drawn, stream_key, smallest, largest):
    index_at = [jax.random.randint(jax.random.fold_in(stream_key, axis), (), 0, length) for axis, length in enumerate(drawn.shape)]
    main_axis = drawn.shape.index(max(drawn.shape))
    neighbour = index_at[:main_axis] + [(index_at[main_axis] + 1) % drawn.shape[main_axis]] + index_at[main_axis + 1:]
    return drawn.at[tuple(index_at)].set(smallest).at[tuple(neighbour)].set(largest)


def cumulative_ranks(count, slope):
    weights = [(1 << 20) // math.isqrt(rank ** slope) + 1 for rank in range(1, count + 1)]
    deviation = 1 + sum(weights) // (1 << 30)
    return np.cumsum(np.array([max(1, weight // deviation) for weight in weights]))


def ranked(key, shape, amount, skew):
    table = cumulative_ranks(amount, skew)
    lot = jax.random.randint(jax.random.fold_in(key, 1), shape, 0, int(table[amount - 1]))
    standing = jnp.searchsorted(jnp.asarray(table, jnp.int32), lot, side="right")
    return jax.random.permutation(jax.random.fold_in(key, 2), amount)[standing].astype(jnp.int32)


def profile(number_of, total, most, lean):
    weights = [(1 << 20) // math.isqrt(rank ** lean) + 1 for rank in range(2, number_of + 1)]
    surplus, holding = total - most - (number_of - 1), [1] * (number_of - 1)
    while surplus > 0:
        movable = [i for i in range(number_of - 1) if holding[i] < most]
        mass, budget = sum([weights[i] for i in movable]), surplus
        for i in movable:
            extra = min(most - holding[i], max(1, budget * weights[i] // mass), surplus)
            holding[i] = holding[i] + extra
            surplus = surplus - extra
    return np.array([most] + holding)


def uneven(rng, count, total, limit, lean):
    if count == 2:
        one = jax.random.randint(rng, (), max(1, total - limit), min(limit, total - 1) + 1)
        return jnp.stack([one, total - one])
    tallies = jnp.asarray(profile(count, total, limit, lean), jnp.int32)
    pairs = (count - 1) // 2
    giver, taker = tallies[1:1 + 2 * pairs:2], tallies[2:2 + 2 * pairs:2]
    room = jnp.minimum(giver - 1, limit - taker)
    moved = jax.random.randint(jax.random.fold_in(rng, 1), (pairs,), 0, 1 << 20) % (room + 1)
    tallies = tallies.at[1:1 + 2 * pairs:2].set(giver - moved).at[2:2 + 2 * pairs:2].set(taker + moved)
    return tallies[jax.random.permutation(jax.random.fold_in(rng, 2), count)]


def setup_inputs(seed: int = 0) -> dict:
    key_list = jax.random.split(jax.random.key(seed), 6)
    umi_counts = draw_umi_counts(jax.random.fold_in(key_list[5], 71), 0)
    cell_donors = set_ends(jax.random.randint(key_list[1], (CELLS,), 0, DONORS), jax.random.fold_in(key_list[1], 1), 0, DONORS - 1).astype(jnp.int32)
    cell_types = set_ends(ranked(key_list[2], (CELLS,), TYPES, 2), jax.random.fold_in(key_list[2], 3), 0, TYPES - 1).astype(jnp.int32)
    live_cells = uneven(key_list[3], N_BATCH, CELLS * 5 // 8, CELL_DEV, 2).astype(jnp.int32)
    dosages = set_ends(jax.random.randint(key_list[4], (DONORS, VARIANTS), 0, 3), jax.random.fold_in(key_list[4], 1), 0, 2).astype(jnp.int32)
    return dict(umi_counts=umi_counts, cell_donors=cell_donors, cell_types=cell_types, live_cells=live_cells, dosages=dosages)


def reference(umi_counts, cell_donors, cell_types, live_cells, dosages):
    cells_total = umi_counts.shape[0]
    total_groups = TYPES * DONORS
    row_index = jnp.arange(cells_total, dtype=jnp.int32)
    alive = row_index % CELL_DEV < live_cells[row_index // CELL_DEV]
    group_ids = jnp.where(alive, cell_types * DONORS + cell_donors, total_groups).astype(jnp.int32)
    rounded = lax.optimization_barrier(umi_counts.astype(jnp.bfloat16)).astype(jnp.float32)
    pseudo = jax.ops.segment_sum(rounded, group_ids, num_segments=total_groups + 1)[:total_groups]
    library = jnp.maximum(lax.optimization_barrier(jnp.sum(pseudo, axis=1)), 1.0)
    logged = jnp.log1p(10000.0 * pseudo / library[:, None]).reshape(TYPES, DONORS, -1)
    centred = logged - lax.optimization_barrier(jnp.mean(logged, axis=1, keepdims=True))
    standard = (centred * lax.rsqrt(lax.optimization_barrier(jnp.mean(centred * centred, axis=1, keepdims=True)) + 1e-06)).astype(jnp.bfloat16)
    genotype = dosages.astype(jnp.float32)
    geno_centred = genotype - lax.optimization_barrier(jnp.mean(genotype, axis=0, keepdims=True))
    geno = (geno_centred * lax.rsqrt(lax.optimization_barrier(jnp.mean(geno_centred * geno_centred, axis=0, keepdims=True)) + 1e-06)).astype(jnp.bfloat16)
    factor = DONORS ** (-0.5)

    def per_type(block):
        return (jnp.dot(block.T, geno, preferred_element_type=jnp.float32) * factor).astype(jnp.bfloat16)
    return lax.map(per_type, standard)
```

```python
import functools

import jax
import jax.numpy as jnp
from jax import lax
from jax.experimental import pallas as pl
from jax.experimental.pallas import tpu as pltpu
from jax.sharding import PartitionSpec as P

TYPES = 24
DONORS = 128
CODE_STEPS = 65535
CODE_SHIFT = 32768


def standardize_dosage(block_dosage):
    genotype = block_dosage.astype(jnp.float32)
    centred = genotype - jnp.mean(genotype, axis=0, keepdims=True)
    return (centred * lax.rsqrt(jnp.mean(centred * centred, axis=0, keepdims=True) + 1e-06)).astype(
        jnp.bfloat16
    )


def add_cells(ids_ref, block_ref, *refs):
    out_ref = refs[-1]
    rows, cells = out_ref.shape[0], block_ref.shape[0]
    columns = lax.broadcasted_iota(jnp.int32, (rows, cells), 0) + pl.program_id(0) * rows
    table = jnp.where(columns == ids_ref[...], 1.0, 0.0).astype(jnp.bfloat16)
    total = jnp.dot(table, block_ref[...], preferred_element_type=jnp.float32)
    if len(refs) == 2:
        total = total + refs[0][...]
    out_ref[...] = total


def group_sums(ids, block, held, total_groups):
    cells, genes = block.shape
    tile = 512
    spec = pl.BlockSpec((tile, genes), lambda i: (i, 0))
    operands = [ids.reshape(1, cells), block] + ([] if held is None else [held])
    return pl.pallas_call(
        add_cells,
        grid=(total_groups // tile,),
        in_specs=[
            pl.BlockSpec((1, cells), lambda i: (0, 0)),
            pl.BlockSpec((cells, genes), lambda i: (0, 0)),
        ]
        + ([] if held is None else [spec]),
        out_specs=spec,
        out_shape=jax.ShapeDtypeStruct((total_groups, genes), jnp.float32),
        input_output_aliases={} if held is None else {2: 0},
        cost_estimate=pl.CostEstimate(
            flops=2 * total_groups * cells * genes,
            bytes_accessed=8 * total_groups * genes + 2 * cells * genes,
            transcendentals=0,
        ),
        name="group_sums",
    )(*operands)


def score_type(scale, pseudo_ref, code_ref, library_ref, geno_ref, out_ref):
    code = (code_ref[...].astype(jnp.int32) + CODE_SHIFT).astype(jnp.float32)
    other = jnp.exp2(code * (1.0 / scale)) - 1.0
    pseudo = pseudo_ref[...] + other
    logged = jnp.log1p(10000.0 * pseudo / library_ref[...])
    centred = logged - jnp.mean(logged, axis=0, keepdims=True)
    standard = (
        centred * lax.rsqrt(jnp.mean(centred * centred, axis=0, keepdims=True) + 1e-06)
    ).astype(jnp.bfloat16)
    product = lax.dot_general(
        standard, geno_ref[...], (((0,), (0,)), ((), ())), preferred_element_type=jnp.float32
    )
    out_ref[0] = (product * DONORS ** (-0.5)).astype(jnp.bfloat16)


def scores_of(pseudo, code, library, geno, scale):
    genes, variants = pseudo.shape[1], geno.shape[1]
    return pl.pallas_call(
        functools.partial(score_type, scale),
        grid=(TYPES,),
        in_specs=[
            pl.BlockSpec((DONORS, genes), lambda t: (t, 0)),
            pl.BlockSpec((DONORS, genes), lambda t: (t, 0)),
            pl.BlockSpec((DONORS, 1), lambda t: (t, 0)),
            pl.BlockSpec((DONORS, variants), lambda t: (0, 0)),
        ],
        out_specs=pl.BlockSpec((1, genes, variants), lambda t: (t, 0, 0)),
        out_shape=jax.ShapeDtypeStruct((TYPES, genes, variants), jnp.bfloat16),
        cost_estimate=pl.CostEstimate(
            flops=2 * TYPES * DONORS * genes * variants,
            bytes_accessed=2 * TYPES * genes * variants,
            transcendentals=0,
        ),
        name="scores_of",
    )(pseudo, code, library, geno)


def on_device(umi_counts, cell_donors, cell_types, live_cells, dosages):
    total_groups = TYPES * DONORS
    cell_slots = umi_counts.shape[0]
    batch_count = lax.axis_size("batch")
    gene_count = lax.axis_size("gene")
    half = batch_count // 2
    genes_local = umi_counts.shape[1] // batch_count
    me = lax.axis_index("batch")
    scale = CODE_STEPS / float((65536 * cell_slots * half).bit_length())

    def swap(x, mask):
        return lax.ppermute(x, "batch", [(i, i ^ mask) for i in range(batch_count)])

    alive = jnp.arange(cell_slots, dtype=jnp.int32) < live_cells[0]
    ids = [jnp.where(alive, cell_types * DONORS + cell_donors, -1)]
    ids += [swap(ids[0], mask) for mask in range(1, half)]

    def counts_for(block):
        part = lax.dynamic_slice_in_dim(umi_counts, block * genes_local, genes_local, 1)
        return part.astype(jnp.bfloat16)

    order = list(range(half - 1, 0, -1))
    far = {mask: swap(counts_for(me ^ mask ^ half), mask) for mask in order}
    near = {mask: swap(counts_for(me ^ mask), mask) for mask in order}

    partial = group_sums(ids[0], counts_for(me ^ half), None, total_groups)
    for mask in range(1, half):
        partial = group_sums(ids[mask], far[mask], partial, total_groups)
    code = jnp.round(jnp.log2(1.0 + partial) * scale).astype(jnp.int32) - CODE_SHIFT
    code = swap(code.astype(jnp.int16), half)

    depth = jnp.sum(umi_counts.astype(jnp.bfloat16).astype(jnp.int32), axis=1)
    depth_all = depth
    for step in range(1, gene_count):
        depth_all = depth_all + lax.ppermute(
            depth, "gene", [(i, (i + step) % gene_count) for i in range(gene_count)]
        )
    groups = jnp.arange(total_groups, dtype=jnp.int32)
    library = jnp.zeros((total_groups,), jnp.float32)
    for mask in range(half):
        cells = swap(depth_all, mask) if mask else depth_all
        library = library + jnp.sum(
            jnp.where(
                ids[mask][:, None] == groups[None, :], cells.astype(jnp.float32)[:, None], 0.0
            ),
            axis=0,
        )
    library = jnp.maximum(library + swap(library, half), 1.0)

    geno_local = standardize_dosage(dosages)
    variants_local = dosages.shape[1]
    geno = jnp.zeros((DONORS, variants_local * batch_count), jnp.bfloat16)
    for mask in range(batch_count):
        piece = swap(geno_local, mask) if mask else geno_local
        geno = lax.dynamic_update_slice_in_dim(geno, piece, (me ^ mask) * variants_local, 1)

    pseudo = group_sums(ids[0], counts_for(me), None, total_groups)
    for mask in range(1, half):
        pseudo = group_sums(ids[mask], near[mask], pseudo, total_groups)
    return scores_of(pseudo, code, library[:, None], geno, scale)


def solution(mesh):
    placed = (P("batch", "gene"), P("batch"), P("batch"), P("batch"), P(None, "batch"))
    return jax.shard_map(
        on_device,
        mesh=mesh,
        in_specs=placed,
        out_specs=P(None, ("gene", "batch"), None),
        check_vma=False,
    )
```

```python
import functools

import jax
import jax.numpy as jnp
from jax import lax
from jax.experimental import pallas as pl
from jax.experimental.pallas import tpu as pltpu
from jax.sharding import PartitionSpec as P

TYPES = 24
DONORS = 128
CODE_STEPS = 65535
CODE_SHIFT = 32768


def standardize_dosage(block_dosage):
    genotype = block_dosage.astype(jnp.float32)
    centred = genotype - jnp.mean(genotype, axis=0, keepdims=True)
    return (centred * lax.rsqrt(jnp.mean(centred * centred, axis=0, keepdims=True) + 1e-06)).astype(
        jnp.bfloat16
    )


def add_cells(scale, with_held, *refs):
    sources = (len(refs) - 1 - with_held) // 2
    out_ref = refs[-1]
    rows, cells = out_ref.shape[0], refs[sources].shape[0]
    columns = lax.broadcasted_iota(jnp.int16, (rows, cells), 0)
    first = pl.program_id(0) * rows
    total = refs[2 * sources][...] if with_held else None
    for ids_ref, block_ref in zip(refs[:sources], refs[sources : 2 * sources]):
        here = jnp.clip(ids_ref[...] - first, -1, rows).astype(jnp.int16)
        here = jnp.broadcast_to(here, (rows, cells))
        table = jnp.where(columns == here, jnp.bfloat16(1.0), jnp.bfloat16(0.0))
        added = jnp.dot(table, block_ref[...], preferred_element_type=jnp.float32)
        total = added if total is None else total + added
    if scale is not None:
        code = jnp.floor(jnp.log2(1.0 + total) * scale + 0.5)
        total = code.astype(jnp.int32) - CODE_SHIFT
    out_ref[...] = total.astype(out_ref.dtype)


def group_sums(ids, blocks, held, total_groups, scale=None):
    cells, genes = blocks[0].shape
    tile = 256
    spec = pl.BlockSpec((tile, genes), lambda i: (i, 0))
    operands = [x.reshape(1, cells) for x in ids] + blocks + ([] if held is None else [held])
    out_type = jnp.float32 if scale is None else jnp.int16
    return pl.pallas_call(
        functools.partial(add_cells, scale, held is not None),
        grid=(total_groups // tile,),
        in_specs=[pl.BlockSpec((1, cells), lambda i: (0, 0)) for _ in ids]
        + [pl.BlockSpec((cells, genes), lambda i: (0, 0)) for _ in blocks]
        + ([] if held is None else [spec]),
        out_specs=spec,
        out_shape=jax.ShapeDtypeStruct((total_groups, genes), out_type),
        cost_estimate=pl.CostEstimate(
            flops=2 * total_groups * cells * genes * len(blocks),
            bytes_accessed=8 * total_groups * genes + 2 * cells * genes * len(blocks),
            transcendentals=0,
        ),
        name="group_sums",
    )(*operands)


def score_type(scale, pseudo_ref, code_ref, rate_ref, geno_ref, out_ref):
    code = (code_ref[...].astype(jnp.int32) + CODE_SHIFT).astype(jnp.float32)
    other = jnp.exp2(code * (1.0 / scale)) - 1.0
    pseudo = pseudo_ref[...] + other
    logged = jnp.log(1.0 + pseudo * rate_ref[...])
    centred = logged - jnp.mean(logged, axis=0, keepdims=True)
    standard = centred * lax.rsqrt(jnp.mean(centred * centred, axis=0, keepdims=True) + 1e-06)
    rows = standard.T.astype(jnp.bfloat16)
    variants = geno_ref.shape[1]
    width = min(variants, 256)
    for lo in range(0, variants, width):
        product = jnp.dot(
            rows, geno_ref[:, lo : lo + width], preferred_element_type=jnp.float32
        )
        out_ref[0, :, lo : lo + width] = (product * DONORS ** (-0.5)).astype(jnp.bfloat16)


def scores_of(pseudo, code, library, geno, scale):
    genes, variants = pseudo.shape[1], geno.shape[1]
    return pl.pallas_call(
        functools.partial(score_type, scale),
        grid=(TYPES,),
        in_specs=[
            pl.BlockSpec((DONORS, genes), lambda t: (t, 0)),
            pl.BlockSpec((DONORS, genes), lambda t: (t, 0)),
            pl.BlockSpec((DONORS, 1), lambda t: (t, 0)),
            pl.BlockSpec((DONORS, variants), lambda t: (0, 0)),
        ],
        out_specs=pl.BlockSpec((1, genes, variants), lambda t: (t, 0, 0)),
        out_shape=jax.ShapeDtypeStruct((TYPES, genes, variants), jnp.bfloat16),
        cost_estimate=pl.CostEstimate(
            flops=2 * TYPES * DONORS * genes * variants,
            bytes_accessed=2 * TYPES * genes * variants,
            transcendentals=0,
        ),
        name="scores_of",
    )(pseudo, code, library, geno)


def on_device(umi_counts, cell_donors, cell_types, live_cells, dosages):
    total_groups = TYPES * DONORS
    cell_slots = umi_counts.shape[0]
    batch_count = lax.axis_size("batch")
    gene_count = lax.axis_size("gene")
    half = batch_count // 2
    genes_local = umi_counts.shape[1] // batch_count
    me = lax.axis_index("batch")
    scale = CODE_STEPS / float((65536 * cell_slots * half).bit_length())

    def swap(x, mask):
        return lax.ppermute(x, "batch", [(i, i ^ mask) for i in range(batch_count)])

    geno = standardize_dosage(dosages)
    bits = batch_count.bit_length() - 1
    for bit in range(bits - 1, -1, -1):
        other = swap(geno, 1 << bit)
        upper = (me >> bit) & 1
        geno = jnp.where(upper == 1, jnp.stack([other, geno]), jnp.stack([geno, other]))
    geno = geno.transpose(*range(bits - 1, -1, -1), bits, bits + 1)
    geno = geno.reshape(batch_count, DONORS, -1).transpose(1, 0, 2).reshape(DONORS, -1)

    alive = jnp.arange(cell_slots, dtype=jnp.int32) < live_cells[0]
    cell_group = jnp.where(alive, cell_types * DONORS + cell_donors, -1)
    depth = jnp.sum(umi_counts.astype(jnp.bfloat16).astype(jnp.int32), axis=1)
    cell_facts = jnp.stack([cell_group, depth])
    facts = [cell_facts] + [swap(cell_facts, mask) for mask in range(1, half)]
    ids = [fact[0] for fact in facts]

    def counts_for(block):
        part = lax.dynamic_slice_in_dim(umi_counts, block * genes_local, genes_local, 1)
        return part.astype(jnp.bfloat16)

    order = list(range(half - 1, 0, -1))
    far_out = [counts_for(me ^ mask ^ half) for mask in order]
    far_out, geno, facts = lax.optimization_barrier((far_out, geno, facts))
    ids = [fact[0] for fact in facts]
    far = {mask: swap(out, mask) for mask, out in zip(order, far_out)}
    near_out = [counts_for(me ^ mask) for mask in order]
    near = {mask: swap(out, mask) for mask, out in zip(order, near_out)}

    partial = None
    pairs = [(low, low + 1) for low in range(0, half, 2)]
    far[0] = counts_for(me ^ half)
    for pair in pairs:
        last = scale if pair == pairs[-1] else None
        partial = group_sums(
            [ids[m] for m in pair], [far[m] for m in pair], partial, total_groups, last
        )
    code = swap(partial, half)

    pseudo = None
    near[0] = counts_for(me)
    quads = [tuple(range(low, low + 4)) for low in range(0, half, 4)]
    for quad in quads:
        pseudo = group_sums([ids[m] for m in quad], [near[m] for m in quad], pseudo, total_groups)

    digits = [
        jnp.stack([((fact[1] >> (8 * d)) & 255).astype(jnp.bfloat16) for d in range(4)], axis=1)
        for fact in facts
    ]
    digits = [jnp.pad(x, ((0, 0), (0, 124))) for x in digits]
    digits, pseudo = lax.optimization_barrier((digits, pseudo))
    digit_sums = group_sums(ids, digits, None, total_groups)
    library = (
        digit_sums[:, 0]
        + 256.0 * digit_sums[:, 1]
        + 65536.0 * digit_sums[:, 2]
        + 16777216.0 * digit_sums[:, 3]
    )
    mine = library
    for step in range(1, gene_count):
        library = library + lax.ppermute(
            mine, "gene", [(i, (i + step) % gene_count) for i in range(gene_count)]
        )
    rate = 10000.0 / jnp.maximum(library + swap(library, half), 1.0)

    return scores_of(pseudo, code, rate[:, None], geno, scale)


def solution(mesh):
    placed = (P("batch", "gene"), P("batch"), P("batch"), P("batch"), P(None, "batch"))
    return jax.shard_map(
        on_device,
        mesh=mesh,
        in_specs=placed,
        out_specs=P(None, ("gene", "batch"), None),
        check_vma=False,
    )
```
